32 devices in a mesh: dp: 8 (over z, y), tp: 4 (over x, core).
Axes of the slice: x: 2, y: 2, z: 4, core: 2. Of those that a mesh axis runs over, the one named last changes fastest.
Arguments:
- queries: bfloat16 [64, 16, 8192], P(('dp', 'tp')), parts along dimension 0, may hold values from -512 to 512
- kv_cache: bfloat16 [64, 8, 384, 256], P(('dp', 'tp')), parts along dimension 0, may hold values from -18 to 18
- lengths: int32 [64], P(('dp', 'tp')), parts along dimension 0, may hold values from 17 to 384, as said below
- residual: bfloat16 [64, 16, 8192], P(('dp', 'tp')), parts along dimension 0, may hold values from -4 to 4
- out_weight: bfloat16 [8192, 8192], P('tp'), may hold values from -0.0625 to 0.0625
- norm_gain: bfloat16 [8192], replicated, may hold values from 0.25 to 1.75
Outputs:
- hidden: bfloat16 [64, 16, 8192], P(('dp', 'tp')), parts along dimension 0
- normed: bfloat16 [64, 16, 8192], P(('dp', 'tp')), parts along dimension 0
The draws below stay inside these ranges and needn't reach their ends.
There are 8 independent parts, one for each index of `dp`. The reference program is written for one: setup_inputs(seed, part) draws one part's arguments, and reference() takes and returns one part's arrays. A program takes and returns all parts, laid end to end along the dimension named above; an argument that names none is the same for every part. Nothing has to cross between parts.
Inputs may be any that keep to these rules, and one draw needn't show every extreme that they name: `lengths`: some sequence of every part has exactly 384 live slots.
All inputs are finite; a program needn't handle non-finite values.
Results may differ from the reference program's by a relative error of at most 0.015.
Values may be sent and summed in bfloat16 or wider, within the bound.
A program may use at most 128 MiB of HBM per device.

```python
import jax
import jax.numpy as jnp
from jax import lax

D = 8192
HEADS = 64
KV_HEADS = 8
HEAD_DIM = 128
DRAFT = 16
LEN = 384
SEQS = 8
N_TP = 4


def draw_queries(key, part):
    normal_part = jnp.clip(jax.random.normal(jax.random.fold_in(key, 11), (SEQS, DRAFT, HEADS * HEAD_DIM), jnp.float32) * 1.5, -9.0, 9.0)
    return normal_part.astype(jnp.bfloat16)


def draw_kv_cache(key, part):
    shape_all = (SEQS, KV_HEADS, LEN, HEAD_DIM)
    key_part = jnp.clip(jax.random.normal(jax.random.fold_in(key, 21), shape_all, jnp.float32), -6.0, 6.0)
    value_part = jnp.clip(jax.random.normal(jax.random.fold_in(key, 22), shape_all, jnp.float32) * 3.0, -18.0, 18.0)
    return jnp.concatenate([key_part, value_part], axis=-1).astype(jnp.bfloat16)


def draw_lengths(key, part):
    drawn = jax.random.randint(jax.random.fold_in(key, 31), (SEQS,), DRAFT + 1, LEN + 1, dtype=jnp.int32)
    return drawn.at[0].set(LEN)


def draw_residual(key, part):
    row_values = jax.random.normal(jax.random.fold_in(key, 41), (SEQS, DRAFT, D), jnp.float32) * 0.5
    return jnp.clip(row_values, -4.0, 4.0).astype(jnp.bfloat16)


def block_scale(own_key, extent, cuts, smallest, top_value):
    loudness, own = 1.0, jax.random.fold_in(own_key, 6)
    for dim, parts in cuts:
        heights = jnp.exp(jax.random.uniform(jax.random.fold_in(own, dim), (parts,), jnp.float32, smallest / len(cuts), top_value / len(cuts)))
        loudness = loudness * jnp.repeat(heights, extent[dim] // parts).reshape([-1 if axis == dim else 1 for axis in range(len(extent))])
    return loudness


def gaussian(key, extent, width, most, shards=(), kind=jnp.bfloat16):
    gain = block_scale(key, extent, shards, -0.22, 0.18) if shards else 1.0
    entries = jax.random.normal(key, extent, jnp.float32) * width * gain
    return jnp.minimum(jnp.maximum(entries, -most), most).astype(kind)


def setup_inputs(seed: int = 0, part: int = 0) -> dict:
    key_list = jax.random.split(jax.random.key(seed), 7)
    own_keys = jax.random.split(jax.random.fold_in(key_list[6], part), 7)
    return {
        "queries": draw_queries(jax.random.fold_in(jax.random.fold_in(key_list[6], part), 71), part),
        "kv_cache": draw_kv_cache(jax.random.fold_in(jax.random.fold_in(key_list[6], part), 71), part),
        "lengths": draw_lengths(jax.random.fold_in(jax.random.fold_in(key_list[6], part), 71), part),
        "residual": draw_residual(jax.random.fold_in(jax.random.fold_in(key_list[6], part), 71), part),
        "out_weight": gaussian(key_list[4], (HEADS * HEAD_DIM, D), (HEADS * HEAD_DIM) ** -0.5, 0.0625, ((0, 4),)),
        "norm_gain": jnp.clip(1.0 + 0.15 * jax.random.normal(key_list[5], (D,), jnp.float32), 0.25, 1.75).astype(jnp.bfloat16),
    }


def attend(queries, kv_cache, lengths):
    seq_count = queries.shape[0]
    per_group = HEADS // KV_HEADS
    grouped = queries.reshape(seq_count, DRAFT, KV_HEADS, per_group, HEAD_DIM).transpose(0, 2, 3, 1, 4)
    grouped = grouped.reshape(seq_count, KV_HEADS, per_group * DRAFT, HEAD_DIM).astype(jnp.float32)
    key_part = kv_cache[..., :HEAD_DIM].astype(jnp.float32)
    value_part = kv_cache[..., HEAD_DIM:].astype(jnp.float32)
    scores = jnp.einsum('skqd,skld->skql', grouped, key_part) * HEAD_DIM ** (-0.5)
    draft_index = jnp.arange(per_group * DRAFT, dtype=jnp.int32) % DRAFT
    visible = lengths[:, None, None, None] - DRAFT + 1 + draft_index[None, None, :, None]
    position = jnp.arange(LEN, dtype=jnp.int32)
    allowed = position[None, None, None, :] < visible
    scores = jnp.where(allowed, scores, -1e+30)
    peak = lax.optimization_barrier(jnp.max(scores, axis=-1, keepdims=True))
    raised = jnp.exp(scores - peak)
    totals = lax.optimization_barrier(jnp.sum(raised, axis=-1, keepdims=True))
    weights = (raised / totals).astype(jnp.bfloat16)
    attended = jnp.einsum('skql,skld->skqd', weights.astype(jnp.float32), value_part).astype(jnp.bfloat16)
    attended = attended.reshape(seq_count, KV_HEADS, per_group, DRAFT, HEAD_DIM).transpose(0, 3, 1, 2, 4)
    return attended.reshape(seq_count, DRAFT, HEADS * HEAD_DIM)

def reference(queries, kv_cache, lengths, residual, out_weight, norm_gain):
    attended = attend(queries, kv_cache, lengths)
    flat_rows = attended.reshape(SEQS * DRAFT, HEADS * HEAD_DIM)
    columns = HEADS * HEAD_DIM // N_TP
    projected = jnp.zeros((SEQS * DRAFT, D), jnp.float32)
    for shard in range(N_TP):
        partial_term = jnp.dot(flat_rows[:, shard * columns:(shard + 1) * columns], out_weight[shard * columns:(shard + 1) * columns], preferred_element_type=jnp.float32)
        projected = projected + lax.optimization_barrier(partial_term.astype(jnp.bfloat16)).astype(jnp.float32)
    summed = residual.astype(jnp.float32) + projected.reshape(SEQS, DRAFT, D)
    hidden = summed.astype(jnp.bfloat16)
    scales = lax.rsqrt(lax.optimization_barrier(jnp.mean(summed * summed, axis=-1, keepdims=True)) + 1e-05)
    normed = (summed * scales * norm_gain.astype(jnp.float32)).astype(jnp.bfloat16)
    return (hidden, normed)
```

```python
import functools
import math

import jax
import jax.numpy as jnp
from jax import lax
from jax.experimental import pallas as pl
from jax.experimental.pallas import tpu as pltpu
from jax.sharding import PartitionSpec as P

CORES = 2
COLUMNS = 1024
LANES = 128
LAG = 2
AHEAD = 5


def block_kernel(
    n,
    split,
    lengths_ref,
    queries_ref,
    kv_ref,
    residual_ref,
    weight_ref,
    gain_ref,
    acc,
    scale_ref,
    wide_gain,
    length_buf,
    gain_buf,
    q_buf,
    kv_buf,
    res_buf,
    w_buf,
    att_send,
    att,
    keep,
    mate_send,
    mate_recv,
    cross_send,
    cross_recv,
    small_sem,
    q_sem,
    kv_sem,
    w_sem,
    att_send_sem,
    att_recv_sem,
    mate_send_sem,
    mate_recv_sem,
    cross_send_sem,
    cross_recv_sem,
):
    chips = n // CORES
    seqs, draft, width = queries_ref.shape
    kv_heads, slots_kv, head_dim = kv_ref.shape[1], kv_ref.shape[2], kv_ref.shape[3] // 2
    heads = width // head_dim
    group = heads // kv_heads
    own_heads = heads // n
    unit_heads = min(own_heads, group)
    units = own_heads // unit_heads
    kv_per_dest = kv_buf.shape[1]
    rows = seqs * draft
    chunks, depth, columns = w_buf.shape
    model = chunks * columns

    early = seqs // 2
    late = seqs - early
    early_rows, late_rows = early * draft, late * draft
    others = chips - 1
    local_at = others * CORES * early_rows
    late_at = local_at + CORES * rows
    att_rows = late_at + others * CORES * late_rows
    mate_local = others * early_rows
    mate_late = mate_local + rows
    mate_rows = mate_late + others * late_rows

    me = lax.axis_index("tp")
    chip, core = me // CORES, me % CORES

    def device(dx, dk):
        return ((chip + dx) % chips) * CORES + (core + dk) % CORES

    def att_row(dx, dk, s):
        if dx == 0:
            return local_at + dk * rows + s * draft
        place = (dx - 1) * CORES + dk
        if s < early:
            return place * early_rows + s * draft
        return late_at + place * late_rows + (s - early) * draft

    remote = [(dx, dk) for dx in range(1, chips) for dk in range(CORES)]
    order = [(dx, dk, s) for s in range(seqs) for dx, dk in remote]
    order += [(0, 1, s) for s in range(seqs)] + [(0, 0, s) for s in range(seqs)]

    barrier = pltpu.get_barrier_semaphore()
    for dx, dk in [(0, 1)] + remote:
        pl.semaphore_signal(
            barrier,
            inc=1,
            device_id={"tp": device(dx, dk)},
            device_id_type=pl.DeviceIdType.MESH,
        )

    def q_copy(s):
        return pltpu.make_async_copy(queries_ref.at[s], q_buf.at[s], q_sem.at[s])

    def kv_copy(step):
        dx, dk, s = order[step]
        first = device(dx, dk) * own_heads // group
        return pltpu.make_async_copy(
            kv_ref.at[s, pl.ds(first, kv_per_dest)], kv_buf.at[step], kv_sem.at[step]
        )

    length_copy = pltpu.make_async_copy(lengths_ref, length_buf, small_sem.at[0])
    gain_copy = pltpu.make_async_copy(gain_ref, gain_buf, small_sem.at[1])
    res_copy = pltpu.make_async_copy(residual_ref, res_buf, small_sem.at[2])
    length_copy.start()
    seen = set()
    for step, (_, _, s) in enumerate(order):
        if s not in seen:
            seen.add(s)
            q_copy(s).start()
        kv_copy(step).start()

    def w_copy(c):
        at = pl.multiple_of(c * columns, LANES)
        return pltpu.make_async_copy(
            weight_ref.at[:, pl.ds(at, columns)], w_buf.at[c], w_sem.at[c]
        )

    length_copy.wait()
    position = lax.broadcasted_iota(jnp.int32, (draft, slots_kv), 1)
    token = lax.broadcasted_iota(jnp.int32, (draft, slots_kv), 0)
    biases = [
        jnp.where(position < length_buf[s] - draft + 1 + token, 0.0, -1e30).astype(jnp.float32)
        for s in range(seqs)
    ]
    factor = head_dim ** (-0.5) * math.log2(math.e)

    def attend(step, u):
        dx, dk, s = order[step]
        kv_at = u if own_heads >= group else 0
        dest = device(dx, dk)
        start = pl.multiple_of((dest * own_heads + u * unit_heads) * head_dim, LANES)
        wide = q_buf[s, :, pl.ds(start, unit_heads * head_dim)]
        q_rows = jnp.concatenate(
            [wide[:, h * head_dim : (h + 1) * head_dim] for h in range(unit_heads)], axis=0
        )
        keys = kv_buf[step, kv_at, :, :head_dim]
        values = kv_buf[step, kv_at, :, head_dim:]
        scores = lax.dot_general(
            q_rows, keys, (((1,), (1,)), ((), ())), preferred_element_type=jnp.float32
        )
        scores = scores.reshape(unit_heads, draft, slots_kv) + biases[s][None]
        peak = jnp.max(scores, axis=-1, keepdims=True)
        raised = jnp.exp2((scores - peak) * factor)
        totals = jnp.sum(raised, axis=-1, keepdims=True)
        out = jnp.dot(
            raised.astype(jnp.bfloat16).reshape(unit_heads * draft, slots_kv),
            values,
            preferred_element_type=jnp.float32,
        )
        return (out * (1.0 / totals).reshape(unit_heads * draft, 1)).astype(jnp.bfloat16)

    def att_copy(dx, dk, s):
        slot = dx * CORES + dk - 1
        if dx == 0:
            recv = 2
        else:
            recv = 0 if s < early else 1
        return pltpu.make_async_remote_copy(
            src_ref=att_send.at[slot, pl.ds(s * draft, draft)],
            dst_ref=att.at[pl.ds(att_row((chips - dx) % chips, dk, s), draft)],
            send_sem=att_send_sem,
            recv_sem=att_recv_sem.at[recv],
            device_id={"tp": device(dx, dk)},
            device_id_type=pl.DeviceIdType.MESH,
        )

    ahead = max(1, chunks * AHEAD // 8) if split else chunks
    waited = set()
    for step, (dx, dk, s) in enumerate(order):
        slot = dx * CORES + dk
        if s not in waited:
            waited.add(s)
            q_copy(s).wait()
        kv_copy(step).wait()
        for c in range(ahead * step // len(order), ahead * (step + 1) // len(order)):
            w_copy(c).start()
        for u in range(units):
            out = attend(step, u)
            for h in range(unit_heads):
                at = (u * unit_heads + h) * head_dim
                piece = out[h * draft : (h + 1) * draft]
                if slot:
                    att_send[slot - 1, s * draft : (s + 1) * draft, at : at + head_dim] = piece
                else:
                    own = att_row(0, 0, s)
                    att[own : own + draft, at : at + head_dim] = piece
        if step == 0:
            pl.semaphore_wait(barrier, n - 1)
        if slot:
            att_copy(dx, dk, s).start()

    def att_arrived(first, count, which):
        block = att.at[pl.ds(first, count)]
        pltpu.make_async_copy(block, block, att_recv_sem.at[which]).wait()

    def mate_copy(first, count, c, which):
        part = pl.ds(first, count)
        return pltpu.make_async_remote_copy(
            src_ref=mate_send.at[c, part],
            dst_ref=mate_recv.at[c, part],
            send_sem=mate_send_sem,
            recv_sem=mate_recv_sem.at[which],
            device_id={"tp": device(0, 1)},
            device_id_type=pl.DeviceIdType.MESH,
        )

    def cross_copy(dx, first, count, c, which):
        part = pl.ds(first, count)
        return pltpu.make_async_remote_copy(
            src_ref=cross_send.at[dx - 1, c, part],
            dst_ref=cross_recv.at[chips - dx - 1, c, part],
            send_sem=cross_send_sem,
            recv_sem=cross_recv_sem.at[which],
            device_id={"tp": device(dx, 0)},
            device_id_type=pl.DeviceIdType.MESH,
        )

    FIRST, REST, ALL = 0, 1, 2
    att_span = {FIRST: (0, late_at), REST: (late_at, att_rows), ALL: (0, att_rows)}
    mate_span = {FIRST: (0, mate_late), REST: (mate_late, mate_rows), ALL: (0, mate_rows)}
    cross_span = {FIRST: (0, early_rows), REST: (early_rows, rows), ALL: (0, rows)}

    def mate_slot(kind, c):
        return c if kind == FIRST else split + c

    def cross_slot(kind, c):
        return 0 if kind == FIRST else 1 + c

    def mate_item(kind, c):
        low, high = mate_span[kind]
        return mate_copy(low, high - low, c, mate_slot(kind, c))

    def multiply(kind, c):
        low, high = att_span[kind]
        product = jnp.dot(att[low:high], w_buf[c], preferred_element_type=jnp.float32)

        def part(first, count):
            return product[first - low : first - low + count]

        for dx in range(1, chips):
            if kind != REST and early:
                at = att_row(dx, 0, 0)
                keep[c, dx - 1, 0:early_rows] = part(at, early_rows)
                to = (dx - 1) * early_rows
                mate_send[c, to : to + early_rows] = part(at + early_rows, early_rows).astype(
                    jnp.bfloat16
                )
            if kind != FIRST:
                at = att_row(dx, 0, early)
                keep[c, dx - 1, early_rows:rows] = part(at, late_rows)
                to = mate_late + (dx - 1) * late_rows
                mate_send[c, to : to + late_rows] = part(at + late_rows, late_rows).astype(
                    jnp.bfloat16
                )
        if kind != REST:
            at = pl.multiple_of(c * columns, LANES)
            acc[:, :, pl.ds(at, columns)] = part(local_at, rows).reshape(seqs, draft, columns)
            mate_send[c, mate_local:mate_late] = part(local_at + rows, rows).astype(jnp.bfloat16)
        mate_item(kind, c).start()

    def pass_on(kind, c):
        mate_item(kind, c).wait_recv()
        low, high = cross_span[kind]
        for dx in range(1, chips):
            if kind != REST and early:
                at = (dx - 1) * early_rows
                both = keep[c, dx - 1, 0:early_rows] + mate_recv[c, at : at + early_rows].astype(
                    jnp.float32
                )
                cross_send[dx - 1, c, 0:early_rows] = both.astype(jnp.bfloat16)
            if kind != FIRST:
                at = mate_late + (dx - 1) * late_rows
                both = keep[c, dx - 1, early_rows:rows] + mate_recv[
                    c, at : at + late_rows
                ].astype(jnp.float32)
                cross_send[dx - 1, c, early_rows:rows] = both.astype(jnp.bfloat16)
            cross_copy(dx, low, high - low, c, cross_slot(kind, c)).start()
        if kind != REST:
            at = pl.multiple_of(c * columns, LANES)
            other = mate_recv[c, mate_local:mate_late].astype(jnp.float32)
            residual = res_buf[:, :, pl.ds(at, columns)].astype(jnp.float32)
            acc[:, :, pl.ds(at, columns)] += other.reshape(seqs, draft, columns) + residual

    def sweep(kind, first, last, before, wait_w):
        lag = min(LAG, last - first)

        def step(c, carry):
            if wait_w:
                w_copy(c).wait()
            if kind == FIRST:

                @pl.when(c + ahead < chunks)
                def _():
                    w_copy(c + ahead).start()

            multiply(kind, c)
            if before is not None:
                kind_before, last_before, lag_before = before

                @pl.when(c - first < lag_before)
                def _():
                    pass_on(kind_before, last_before - lag_before + c - first)

            @pl.when(c - first >= lag)
            def _():
                pass_on(kind, c - lag)

            return carry

        lax.fori_loop(first, last, step, 0)
        done = 0 if before is None else min(before[2], last - first)
        if before is not None:
            for c in range(before[1] - before[2] + done, before[1]):
                pass_on(before[0], c)
        return kind, last, lag

    res_copy.start()
    gain_copy.start()
    before = None
    att_arrived(local_at + rows, rows, 2)
    if early:
        att_arrived(0, local_at, 0)
    res_copy.wait()
    if split:
        before = sweep(FIRST, 0, split, None, True)
    att_arrived(late_at, att_rows - late_at, 1)
    if split < chunks:
        before = sweep(ALL, split, chunks, before, True)
    if split:
        before = sweep(REST, 0, split, before, False)
    for c in range(before[1] - before[2], before[1]):
        pass_on(before[0], c)

    def arrived(kind, c, count):
        low, high = cross_span[kind]
        block = cross_recv.at[:, pl.ds(c, count), pl.ds(low, high - low)]
        pltpu.make_async_copy(block, block, cross_recv_sem.at[cross_slot(kind, c)]).wait()

    def collect(kind, c, squares):
        low, high = cross_span[kind]
        at = pl.multiple_of(c * columns, LANES)
        s0, s1 = low // draft, high // draft
        total = acc[s0:s1, :, pl.ds(at, columns)]
        for dx in range(1, chips):
            part = cross_recv[dx - 1, c, low:high].astype(jnp.float32)
            total = total + part.reshape(s1 - s0, draft, columns)
        acc[s0:s1, :, pl.ds(at, columns)] = total
        for tile in range(columns // LANES):
            part = total[:, :, tile * LANES : (tile + 1) * LANES]
            squares = squares + part * part
        return squares

    gain_copy.wait()
    wide_gain[...] = gain_buf[...].astype(jnp.float32)

    def finish(kind, c, squares):
        arrived(kind, c, 1)
        return collect(kind, c, squares)

    def gather(kind, first, last, squares):
        return lax.fori_loop(first, last, functools.partial(finish, kind), squares)

    squares = jnp.zeros((seqs, draft, LANES), jnp.float32)
    if split:
        arrived(FIRST, 0, split)
        first = lax.fori_loop(0, split, functools.partial(collect, FIRST), squares[:early])
    squares = gather(ALL, split, chunks, squares)
    if split:
        last = gather(REST, 0, split, squares[early:])
        squares = jnp.concatenate([first + squares[:early], last], axis=0)
    mean = jnp.sum(squares, axis=-1, keepdims=True) / model
    scale_ref[...] = jnp.broadcast_to(lax.rsqrt(mean + 1e-05), scale_ref.shape)

    pltpu.make_async_copy(att_send, att_send, att_send_sem).wait()
    pltpu.make_async_copy(mate_send, mate_send, mate_send_sem).wait()
    pltpu.make_async_copy(cross_send, cross_send, cross_send_sem).wait()


def on_device(n, queries, kv_cache, lengths, residual, out_weight, norm_gain):
    seqs, draft, width = queries.shape
    kv_heads, slots_kv, pair_dim = kv_cache.shape[1:]
    head_dim = pair_dim // 2
    heads = width // head_dim
    depth, model = out_weight.shape
    chips = n // CORES
    others = max(1, chips - 1)
    rows = seqs * draft
    columns = math.gcd(model, COLUMNS)
    chunks = model // columns
    split = chunks // 2 if seqs > 1 and chips > 1 else 0
    kv_per_dest = max(1, kv_heads // n)
    bf16, f32 = jnp.bfloat16, jnp.float32
    dma = pltpu.SemaphoreType.DMA
    summed, scale, gain = pl.pallas_call(
        functools.partial(block_kernel, n, split),
        out_shape=(
            pltpu.VMEM(residual.shape, f32),
            pltpu.VMEM((seqs, draft, LANES), f32),
            pltpu.VMEM(norm_gain.shape, f32),
        ),
        in_specs=[pl.BlockSpec(memory_space=pl.ANY)] * 6,
        out_specs=[pl.BlockSpec(memory_space=pltpu.VMEM)] * 3,
        scratch_shapes=[
            pltpu.SMEM(lengths.shape, jnp.int32),
            pltpu.VMEM(norm_gain.shape, bf16),
            pltpu.VMEM(queries.shape, bf16),
            pltpu.VMEM((n * seqs, kv_per_dest, slots_kv, pair_dim), bf16),
            pltpu.VMEM(residual.shape, bf16),
            pltpu.VMEM((chunks, depth, columns), bf16),
            pltpu.VMEM((n - 1, rows, depth), bf16),
            pltpu.VMEM((n * rows, depth), bf16),
            pltpu.VMEM((chunks, others, rows, columns), f32),
            pltpu.VMEM((chunks, chips * rows, columns), bf16),
            pltpu.VMEM((chunks, chips * rows, columns), bf16),
            pltpu.VMEM((others, chunks, rows, columns), bf16),
            pltpu.VMEM((others, chunks, rows, columns), bf16),
            dma((3,)),
            dma((seqs,)),
            dma((n * seqs,)),
            dma((chunks,)),
            dma,
            dma((3,)),
            dma,
            dma((chunks + split,)),
            dma,
            dma((1 + chunks,)),
        ],
        compiler_params=pltpu.CompilerParams(
            collective_id=0, has_side_effects=True, vmem_limit_bytes=56 * 1024 * 1024
        ),
    )(lengths, queries, kv_cache, residual, out_weight, norm_gain)
    normed = summed * scale[:, :, :1] * gain
    return summed.astype(bf16), normed.astype(bf16)


def solution(mesh):
    return jax.shard_map(
        functools.partial(on_device, mesh.shape["tp"]),
        mesh=mesh,
        in_specs=(
            P(("dp", "tp"), None, None),
            P(("dp", "tp"), None, None, None),
            P(("dp", "tp")),
            P(("dp", "tp"), None, None),
            P("tp", None),
            P(),
        ),
        out_specs=(P(("dp", "tp"), None, None), P(("dp", "tp"), None, None)),
        check_vma=False,
    )
```

```python
import functools
import math

import jax
import jax.numpy as jnp
from jax import lax
from jax.experimental import pallas as pl
from jax.experimental.pallas import tpu as pltpu
from jax.sharding import PartitionSpec as P

CORES = 2
COLUMNS = 1024
LANES = 128
LAG = 2


def block_kernel(
    n,
    split,
    lengths_ref,
    queries_ref,
    kv_ref,
    residual_ref,
    weight_ref,
    gain_ref,
    acc,
    scale_ref,
    wide_gain,
    length_buf,
    gain_buf,
    q_buf,
    kv_buf,
    res_buf,
    w_buf,
    att_send,
    att,
    keep,
    mate_send,
    mate_recv,
    cross_send,
    cross_recv,
    small_sem,
    q_sem,
    kv_sem,
    w_sem,
    att_send_sem,
    att_recv_sem,
    mate_send_sem,
    mate_recv_sem,
    cross_send_sem,
    cross_recv_sem,
):
    chips = n // CORES
    seqs, draft, width = queries_ref.shape
    kv_heads, slots_kv, head_dim = kv_ref.shape[1], kv_ref.shape[2], kv_ref.shape[3] // 2
    heads = width // head_dim
    group = heads // kv_heads
    own_heads = heads // n
    unit_heads = min(own_heads, group)
    units = own_heads // unit_heads
    kv_per_dest = kv_buf.shape[1]
    rows = seqs * draft
    chunks, depth, columns = w_buf.shape
    model = chunks * columns

    early = seqs // 2
    late = seqs - early
    early_rows, late_rows = early * draft, late * draft
    others = chips - 1
    local_at = others * CORES * early_rows
    late_at = local_at + CORES * rows
    att_rows = late_at + others * CORES * late_rows
    mate_local = others * early_rows
    mate_late = mate_local + rows
    mate_rows = mate_late + others * late_rows

    me = lax.axis_index("tp")
    chip, core = me // CORES, me % CORES

    def device(dx, dk):
        return ((chip + dx) % chips) * CORES + (core + dk) % CORES

    def att_row(dx, dk, s):
        if dx == 0:
            return local_at + dk * rows + s * draft
        place = (dx - 1) * CORES + dk
        if s < early:
            return place * early_rows + s * draft
        return late_at + place * late_rows + (s - early) * draft

    remote = [(dx, dk) for dx in range(1, chips) for dk in range(CORES)]
    order = [(dx, dk, s) for s in range(seqs) for dx, dk in remote]
    order += [(0, 1, s) for s in range(seqs)] + [(0, 0, s) for s in range(seqs)]

    barrier = pltpu.get_barrier_semaphore()
    for dx, dk in [(0, 1)] + remote:
        pl.semaphore_signal(
            barrier,
            inc=1,
            device_id={"tp": device(dx, dk)},
            device_id_type=pl.DeviceIdType.MESH,
        )

    def q_copy(s):
        return pltpu.make_async_copy(queries_ref.at[s], q_buf.at[s], q_sem.at[s])

    def kv_copy(step):
        dx, dk, s = order[step]
        first = device(dx, dk) * own_heads // group
        return pltpu.make_async_copy(
            kv_ref.at[s, pl.ds(first, kv_per_dest)], kv_buf.at[step], kv_sem.at[step]
        )

    length_copy = pltpu.make_async_copy(lengths_ref, length_buf, small_sem.at[0])
    gain_copy = pltpu.make_async_copy(gain_ref, gain_buf, small_sem.at[1])
    res_copy = pltpu.make_async_copy(residual_ref, res_buf, small_sem.at[2])
    length_copy.start()
    seen = set()
    for step, (_, _, s) in enumerate(order):
        if s not in seen:
            seen.add(s)
            q_copy(s).start()
        kv_copy(step).start()

    def w_copy(c):
        at = pl.multiple_of(c * columns, LANES)
        return pltpu.make_async_copy(
            weight_ref.at[:, pl.ds(at, columns)], w_buf.at[c], w_sem.at[c]
        )

    length_copy.wait()
    position = lax.broadcasted_iota(jnp.int32, (draft, slots_kv), 1)
    token = lax.broadcasted_iota(jnp.int32, (draft, slots_kv), 0)
    biases = [
        jnp.where(position < length_buf[s] - draft + 1 + token, 0.0, -1e30).astype(jnp.float32)
        for s in range(seqs)
    ]
    factor = head_dim ** (-0.5) * math.log2(math.e)

    def score(step, u):
        dx, dk, s = order[step]
        kv_at = u if own_heads >= group else 0
        dest = device(dx, dk)
        start = pl.multiple_of((dest * own_heads + u * unit_heads) * head_dim, LANES)
        wide = q_buf[s, :, pl.ds(start, unit_heads * head_dim)]
        q_rows = jnp.concatenate(
            [wide[:, h * head_dim : (h + 1) * head_dim] for h in range(unit_heads)], axis=0
        )
        keys = kv_buf[step, kv_at, :, :head_dim]
        scores = lax.dot_general(
            q_rows, keys, (((1,), (1,)), ((), ())), preferred_element_type=jnp.float32
        )
        return scores.reshape(unit_heads, draft, slots_kv) + biases[s][None]

    def weigh(scores):
        peak = jnp.max(scores, axis=-1, keepdims=True)
        raised = jnp.exp2((scores - peak) * factor)
        return raised.astype(jnp.bfloat16).reshape(unit_heads * draft, slots_kv)

    def mix(step, u, weights):
        kv_at = u if own_heads >= group else 0
        values = kv_buf[step, kv_at, :, head_dim:]
        both = jnp.concatenate([values, jnp.ones_like(values)], axis=1)
        out = jnp.dot(weights, both, preferred_element_type=jnp.float32)
        return (out[:, :head_dim] / out[:, head_dim:]).astype(jnp.bfloat16)

    def attend_all(items):
        scores = [score(*item) for item in items]
        weights = [weigh(x) for x in scores]
        return [(item, mix(*item, x)) for item, x in zip(items, weights)]

    def att_copy(dx, dk, s):
        slot = dx * CORES + dk - 1
        if dx == 0:
            recv = 2
        else:
            recv = 0 if s < early else 1
        return pltpu.make_async_remote_copy(
            src_ref=att_send.at[slot, pl.ds(s * draft, draft)],
            dst_ref=att.at[pl.ds(att_row((chips - dx) % chips, dk, s), draft)],
            send_sem=att_send_sem,
            recv_sem=att_recv_sem.at[recv],
            device_id={"tp": device(dx, dk)},
            device_id_type=pl.DeviceIdType.MESH,
        )

    for c in range(split or chunks):
        w_copy(c).start()
    far = sum(1 for dx, _, _ in order if dx)
    blocks = [[step] for step in range(min(2, far))]
    blocks += [list(range(step, min(step + 2, far))) for step in range(2, far, 2)]
    blocks.append(list(range(far, len(order))))
    waited = set()
    for block in blocks:
        for step in block:
            s = order[step][2]
            if s not in waited:
                waited.add(s)
                q_copy(s).wait()
            kv_copy(step).wait()
        done = attend_all([(step, u) for step in block for u in range(units)])
        for (step, u), out in done:
            dx, dk, s = order[step]
            slot = dx * CORES + dk
            for h in range(unit_heads):
                at = (u * unit_heads + h) * head_dim
                piece = out[h * draft : (h + 1) * draft]
                if slot:
                    att_send[slot - 1, s * draft : (s + 1) * draft, at : at + head_dim] = piece
                else:
                    own = att_row(0, 0, s)
                    att[own : own + draft, at : at + head_dim] = piece
        if 0 in block:
            pl.semaphore_wait(barrier, n - 1)
        for step in block:
            if order[step][0] or order[step][1]:
                att_copy(*order[step]).start()

    def att_arrived(first, count, which):
        block = att.at[pl.ds(first, count)]
        pltpu.make_async_copy(block, block, att_recv_sem.at[which]).wait()

    def mate_copy(first, count, c, which):
        part = pl.ds(first, count)
        return pltpu.make_async_remote_copy(
            src_ref=mate_send.at[c, part],
            dst_ref=mate_recv.at[c, part],
            send_sem=mate_send_sem,
            recv_sem=mate_recv_sem.at[which],
            device_id={"tp": device(0, 1)},
            device_id_type=pl.DeviceIdType.MESH,
        )

    def cross_copy(dx, first, count, c, which):
        part = pl.ds(first, count)
        return pltpu.make_async_remote_copy(
            src_ref=cross_send.at[dx - 1, c, part],
            dst_ref=cross_recv.at[chips - dx - 1, c, part],
            send_sem=cross_send_sem,
            recv_sem=cross_recv_sem.at[which],
            device_id={"tp": device(dx, 0)},
            device_id_type=pl.DeviceIdType.MESH,
        )

    FIRST, REST, ALL = 0, 1, 2
    att_span = {FIRST: (0, late_at), REST: (late_at, att_rows), ALL: (0, att_rows)}
    mate_span = {FIRST: (0, mate_late), REST: (mate_late, mate_rows), ALL: (0, mate_rows)}
    cross_span = {FIRST: (0, early_rows), REST: (early_rows, rows), ALL: (0, rows)}

    def mate_slot(kind, c):
        return c if kind == FIRST else split + c

    def cross_slot(kind, c):
        return 0 if kind == FIRST else 1 + c

    def mate_item(kind, c):
        low, high = mate_span[kind]
        return mate_copy(low, high - low, c, mate_slot(kind, c))

    def multiply(kind, c):
        low, high = att_span[kind]
        product = jnp.dot(att[low:high], w_buf[c], preferred_element_type=jnp.float32)

        def part(first, count):
            return product[first - low : first - low + count]

        for dx in range(1, chips):
            if kind != REST and early:
                at = att_row(dx, 0, 0)
                keep[c, dx - 1, 0:early_rows] = part(at, early_rows)
                to = (dx - 1) * early_rows
                mate_send[c, to : to + early_rows] = part(at + early_rows, early_rows).astype(
                    jnp.bfloat16
                )
            if kind != FIRST:
                at = att_row(dx, 0, early)
                keep[c, dx - 1, early_rows:rows] = part(at, late_rows)
                to = mate_late + (dx - 1) * late_rows
                mate_send[c, to : to + late_rows] = part(at + late_rows, late_rows).astype(
                    jnp.bfloat16
                )
        if kind != REST:
            at = pl.multiple_of(c * columns, LANES)
            acc[:, :, pl.ds(at, columns)] = part(local_at, rows).reshape(seqs, draft, columns)
            mate_send[c, mate_local:mate_late] = part(local_at + rows, rows).astype(jnp.bfloat16)
        mate_item(kind, c).start()

    def pass_on(kind, c):
        mate_item(kind, c).wait_recv()
        low, high = cross_span[kind]
        for dx in range(1, chips):
            if kind != REST and early:
                at = (dx - 1) * early_rows
                both = keep[c, dx - 1, 0:early_rows] + mate_recv[c, at : at + early_rows].astype(
                    jnp.float32
                )
                cross_send[dx - 1, c, 0:early_rows] = both.astype(jnp.bfloat16)
            if kind != FIRST:
                at = mate_late + (dx - 1) * late_rows
                both = keep[c, dx - 1, early_rows:rows] + mate_recv[
                    c, at : at + late_rows
                ].astype(jnp.float32)
                cross_send[dx - 1, c, early_rows:rows] = both.astype(jnp.bfloat16)
            cross_copy(dx, low, high - low, c, cross_slot(kind, c)).start()
        if kind != REST:
            at = pl.multiple_of(c * columns, LANES)
            other = mate_recv[c, mate_local:mate_late].astype(jnp.float32)
            residual = res_buf[:, :, pl.ds(at, columns)].astype(jnp.float32)
            acc[:, :, pl.ds(at, columns)] += other.reshape(seqs, draft, columns) + residual

    res_copy.start()
    gain_copy.start()
    att_arrived(local_at + rows, rows, 2)
    if early:
        att_arrived(0, local_at, 0)
    res_copy.wait()

    def sweep(kind, first, last, pending, wait_late):
        lag = min(LAG, last - first)

        def step(c, carry):
            for k, (kind_before, c_before) in enumerate(pending):

                @pl.when(c - first == k)
                def _():
                    pass_on(kind_before, c_before)

            @pl.when(c - first >= lag)
            def _():
                pass_on(kind, c - lag)

            if wait_late:

                @pl.when(c == first)
                def _():
                    att_arrived(late_at, att_rows - late_at, 1)

            if kind != REST:
                w_copy(c).wait()
                if split:
                    later = split + c - jnp.minimum(c, 1)

                    @pl.when((c != 1) & (later < chunks))
                    def _():
                        w_copy(later).start()

            multiply(kind, c)
            return carry

        lax.fori_loop(first, last, step, 0)
        return [(kind, c) for c in range(last - lag, last)]

    sweeps = [(FIRST, 0, split), (ALL, split, chunks), (REST, 0, split)]
    sweeps = [x for x in sweeps if x[1] < x[2]]
    pending = []
    for index, (kind, low, high) in enumerate(sweeps):
        late_now = kind != FIRST and all(x[0] == FIRST for x in sweeps[:index])
        pending = sweep(kind, low, high, pending, late_now)
    for kind, c in pending:
        pass_on(kind, c)

    def arrived(kind, c, count):
        low, high = cross_span[kind]
        block = cross_recv.at[:, pl.ds(c, count), pl.ds(low, high - low)]
        pltpu.make_async_copy(block, block, cross_recv_sem.at[cross_slot(kind, c)]).wait()

    def collect(kind, c, squares):
        low, high = cross_span[kind]
        at = pl.multiple_of(c * columns, LANES)
        s0, s1 = low // draft, high // draft
        total = acc[s0:s1, :, pl.ds(at, columns)]
        for dx in range(1, chips):
            part = cross_recv[dx - 1, c, low:high].astype(jnp.float32)
            total = total + part.reshape(s1 - s0, draft, columns)
        acc[s0:s1, :, pl.ds(at, columns)] = total
        for tile in range(columns // LANES):
            part = total[:, :, tile * LANES : (tile + 1) * LANES]
            squares = squares + part * part
        return squares

    gain_copy.wait()
    wide_gain[...] = gain_buf[...].astype(jnp.float32)

    def finish(kind, c, squares):
        arrived(kind, c, 1)
        return collect(kind, c, squares)

    sums = {
        FIRST: jnp.zeros((early, draft, LANES), jnp.float32) if early else None,
        REST: jnp.zeros((late, draft, LANES), jnp.float32),
        ALL: jnp.zeros((seqs, draft, LANES), jnp.float32),
    }
    for kind, low, high in sweeps:
        if kind == FIRST:
            arrived(FIRST, 0, split)
        do = collect if kind == FIRST else finish
        sums[kind] = lax.fori_loop(low, high, functools.partial(do, kind), sums[kind])
    squares = sums[ALL]
    if split:
        squares = squares + jnp.concatenate([sums[FIRST], sums[REST]], axis=0)
    mean = jnp.sum(squares, axis=-1, keepdims=True) / model
    scale_ref[...] = jnp.broadcast_to(lax.rsqrt(mean + 1e-05), scale_ref.shape)

    pltpu.make_async_copy(att_send, att_send, att_send_sem).wait()
    pltpu.make_async_copy(mate_send, mate_send, mate_send_sem).wait()
    pltpu.make_async_copy(cross_send, cross_send, cross_send_sem).wait()


def on_device(n, queries, kv_cache, lengths, residual, out_weight, norm_gain):
    seqs, draft, width = queries.shape
    kv_heads, slots_kv, pair_dim = kv_cache.shape[1:]
    head_dim = pair_dim // 2
    heads = width // head_dim
    depth, model = out_weight.shape
    chips = n // CORES
    others = max(1, chips - 1)
    rows = seqs * draft
    columns = math.gcd(model, COLUMNS)
    chunks = model // columns
    split = chunks // 2 if seqs > 1 and chips > 1 and chunks % 2 == 0 else 0
    kv_per_dest = max(1, kv_heads // n)
    bf16, f32 = jnp.bfloat16, jnp.float32
    dma = pltpu.SemaphoreType.DMA
    summed, scale, gain = pl.pallas_call(
        functools.partial(block_kernel, n, split),
        out_shape=(
            pltpu.VMEM(residual.shape, f32),
            pltpu.VMEM((seqs, draft, LANES), f32),
            pltpu.VMEM(norm_gain.shape, f32),
        ),
        in_specs=[pl.BlockSpec(memory_space=pl.ANY)] * 6,
        out_specs=[pl.BlockSpec(memory_space=pltpu.VMEM)] * 3,
        scratch_shapes=[
            pltpu.SMEM(lengths.shape, jnp.int32),
            pltpu.VMEM(norm_gain.shape, bf16),
            pltpu.VMEM(queries.shape, bf16),
            pltpu.VMEM((n * seqs, kv_per_dest, slots_kv, pair_dim), bf16),
            pltpu.VMEM(residual.shape, bf16),
            pltpu.VMEM((chunks, depth, columns), bf16),
            pltpu.VMEM((n - 1, rows, depth), bf16),
            pltpu.VMEM((n * rows, depth), bf16),
            pltpu.VMEM((chunks, others, rows, columns), f32),
            pltpu.VMEM((chunks, chips * rows, columns), bf16),
            pltpu.VMEM((chunks, chips * rows, columns), bf16),
            pltpu.VMEM((others, chunks, rows, columns), bf16),
            pltpu.VMEM((others, chunks, rows, columns), bf16),
            dma((3,)),
            dma((seqs,)),
            dma((n * seqs,)),
            dma((chunks,)),
            dma,
            dma((3,)),
            dma,
            dma((chunks + split,)),
            dma,
            dma((1 + chunks,)),
        ],
        compiler_params=pltpu.CompilerParams(
            collective_id=0, has_side_effects=True, vmem_limit_bytes=56 * 1024 * 1024
        ),
    )(lengths, queries, kv_cache, residual, out_weight, norm_gain)
    normed = summed * scale[:, :, :1] * gain
    return summed.astype(bf16), normed.astype(bf16)


def solution(mesh):
    return jax.shard_map(
        functools.partial(on_device, mesh.shape["tp"]),
        mesh=mesh,
        in_specs=(
            P(("dp", "tp"), None, None),
            P(("dp", "tp"), None, None, None),
            P(("dp", "tp")),
            P(("dp", "tp"), None, None),
            P("tp", None),
            P(),
        ),
        out_specs=(P(("dp", "tp"), None, None), P(("dp", "tp"), None, None)),
        check_vma=False,
    )
```

```python
import functools
import math

import jax
import jax.numpy as jnp
from jax import lax
from jax.experimental import pallas as pl
from jax.experimental.pallas import tpu as pltpu
from jax.sharding import PartitionSpec as P

CORES = 2
COLUMNS = 1024
LANES = 128
LAG = 2


def block_kernel(
    n,
    split,
    lengths_ref,
    queries_ref,
    kv_ref,
    residual_ref,
    weight_ref,
    gain_ref,
    acc,
    scale_ref,
    wide_gain,
    length_buf,
    gain_buf,
    q_buf,
    kv_buf,
    res_buf,
    w_buf,
    att_send,
    att,
    keep,
    mate_send,
    mate_recv,
    cross_send,
    cross_recv,
    small_sem,
    q_sem,
    kv_sem,
    w_sem,
    att_send_sem,
    att_recv_sem,
    mate_send_sem,
    mate_recv_sem,
    cross_send_sem,
    cross_recv_sem,
):
    chips = n // CORES
    seqs, draft, width = queries_ref.shape
    kv_heads, slots_kv, head_dim = kv_ref.shape[1], kv_ref.shape[2], kv_ref.shape[3] // 2
    heads = width // head_dim
    group = heads // kv_heads
    own_heads = heads // n
    unit_heads = min(own_heads, group)
    units = own_heads // unit_heads
    kv_per_dest = kv_buf.shape[1]
    rows = seqs * draft
    chunks, depth, columns = w_buf.shape
    model = chunks * columns

    early = seqs // 2
    late = seqs - early
    early_rows, late_rows = early * draft, late * draft
    others = chips - 1
    local_at = others * CORES * early_rows
    late_at = local_at + CORES * rows
    att_rows = late_at + others * CORES * late_rows
    mate_local = others * early_rows
    mate_late = mate_local + rows
    mate_rows = mate_late + others * late_rows

    me = lax.axis_index("tp")
    chip, core = me // CORES, me % CORES

    def device(dx, dk):
        return ((chip + dx) % chips) * CORES + (core + dk) % CORES

    def att_row(dx, dk, s):
        if dx == 0:
            return local_at + dk * rows + s * draft
        place = (dx - 1) * CORES + dk
        if s < early:
            return place * early_rows + s * draft
        return late_at + place * late_rows + (s - early) * draft

    remote = [(dx, dk) for dx in range(1, chips) for dk in range(CORES)]
    order = [(dx, dk, s) for s in range(seqs) for dx, dk in remote]
    order += [(0, 1, s) for s in range(seqs)] + [(0, 0, s) for s in range(seqs)]

    barrier = pltpu.get_barrier_semaphore()
    for dx, dk in [(0, 1)] + remote:
        pl.semaphore_signal(
            barrier,
            inc=1,
            device_id={"tp": device(dx, dk)},
            device_id_type=pl.DeviceIdType.MESH,
        )

    def q_copy(s):
        return pltpu.make_async_copy(queries_ref.at[s], q_buf.at[s], q_sem.at[s])

    def kv_copy(step):
        dx, dk, s = order[step]
        first = device(dx, dk) * own_heads // group
        return pltpu.make_async_copy(
            kv_ref.at[s, pl.ds(first, kv_per_dest)], kv_buf.at[step], kv_sem.at[step]
        )

    length_copy = pltpu.make_async_copy(lengths_ref, length_buf, small_sem.at[0])
    gain_copy = pltpu.make_async_copy(gain_ref, gain_buf, small_sem.at[1])
    res_copy = pltpu.make_async_copy(residual_ref, res_buf, small_sem.at[2])
    length_copy.start()
    seen = set()
    for step, (_, _, s) in enumerate(order):
        if s not in seen:
            seen.add(s)
            q_copy(s).start()
        kv_copy(step).start()

    def w_copy(c):
        at = pl.multiple_of(c * columns, LANES)
        return pltpu.make_async_copy(
            weight_ref.at[:, pl.ds(at, columns)], w_buf.at[c], w_sem.at[c]
        )

    length_copy.wait()
    position = lax.broadcasted_iota(jnp.int32, (draft, slots_kv), 1)
    token = lax.broadcasted_iota(jnp.int32, (draft, slots_kv), 0)
    biases = [
        jnp.where(position < length_buf[s] - draft + 1 + token, 0.0, -1e30).astype(jnp.float32)
        for s in range(seqs)
    ]
    factor = head_dim ** (-0.5) * math.log2(math.e)

    def score(step, u):
        dx, dk, s = order[step]
        kv_at = u if own_heads >= group else 0
        dest = device(dx, dk)
        start = pl.multiple_of((dest * own_heads + u * unit_heads) * head_dim, LANES)
        wide = q_buf[s, :, pl.ds(start, unit_heads * head_dim)]
        q_rows = jnp.concatenate(
            [wide[:, h * head_dim : (h + 1) * head_dim] for h in range(unit_heads)], axis=0
        )
        keys = kv_buf[step, kv_at, :, :head_dim]
        scores = lax.dot_general(
            q_rows, keys, (((1,), (1,)), ((), ())), preferred_element_type=jnp.float32
        )
        return scores.reshape(unit_heads, draft, slots_kv) + biases[s][None]

    def weigh(scores):
        peak = jnp.max(scores, axis=-1, keepdims=True)
        raised = jnp.exp2((scores - peak) * factor)
        return raised.astype(jnp.bfloat16).reshape(unit_heads * draft, slots_kv)

    def mix(step, u, weights):
        kv_at = u if own_heads >= group else 0
        values = kv_buf[step, kv_at, :, head_dim:]
        both = jnp.concatenate([values, jnp.ones_like(values)], axis=1)
        out = jnp.dot(weights, both, preferred_element_type=jnp.float32)
        return (out[:, :head_dim] / out[:, head_dim:]).astype(jnp.bfloat16)

    def attend_all(items):
        scores = [score(*item) for item in items]
        weights = [weigh(x) for x in scores]
        return [(item, mix(*item, x)) for item, x in zip(items, weights)]

    def att_copy(dx, dk, s):
        slot = dx * CORES + dk - 1
        if dx == 0:
            recv = 2
        else:
            recv = 0 if s < early else 1
        return pltpu.make_async_remote_copy(
            src_ref=att_send.at[slot, pl.ds(s * draft, draft)],
            dst_ref=att.at[pl.ds(att_row((chips - dx) % chips, dk, s), draft)],
            send_sem=att_send_sem,
            recv_sem=att_recv_sem.at[recv],
            device_id={"tp": device(dx, dk)},
            device_id_type=pl.DeviceIdType.MESH,
        )

    for c in range(split or chunks):
        w_copy(c).start()
    far = sum(1 for dx, _, _ in order if dx)
    blocks = [[step] for step in range(min(2, far))]
    blocks += [list(range(step, min(step + 2, far))) for step in range(2, far, 2)]
    blocks.append(list(range(far, len(order))))
    waited = set()
    for block in blocks:
        for step in block:
            s = order[step][2]
            if s not in waited:
                waited.add(s)
                q_copy(s).wait()
            kv_copy(step).wait()
        done = attend_all([(step, u) for step in block for u in range(units)])
        for (step, u), out in done:
            dx, dk, s = order[step]
            slot = dx * CORES + dk
            for h in range(unit_heads):
                at = (u * unit_heads + h) * head_dim
                piece = out[h * draft : (h + 1) * draft]
                if slot:
                    att_send[slot - 1, s * draft : (s + 1) * draft, at : at + head_dim] = piece
                else:
                    own = att_row(0, 0, s)
                    att[own : own + draft, at : at + head_dim] = piece
        if 0 in block:
            pl.semaphore_wait(barrier, n - 1)
        for step in block:
            if order[step][0] or order[step][1]:
                att_copy(*order[step]).start()

    def att_arrived(first, count, which):
        block = att.at[pl.ds(first, count)]
        pltpu.make_async_copy(block, block, att_recv_sem.at[which]).wait()

    def mate_copy(first, count, c, which):
        part = pl.ds(first, count)
        return pltpu.make_async_remote_copy(
            src_ref=mate_send.at[c, part],
            dst_ref=mate_recv.at[c, part],
            send_sem=mate_send_sem,
            recv_sem=mate_recv_sem.at[which],
            device_id={"tp": device(0, 1)},
            device_id_type=pl.DeviceIdType.MESH,
        )

    def cross_copy(dx, first, count, c, which):
        part = pl.ds(first, count)
        return pltpu.make_async_remote_copy(
            src_ref=cross_send.at[dx - 1, c, part],
            dst_ref=cross_recv.at[chips - dx - 1, c, part],
            send_sem=cross_send_sem,
            recv_sem=cross_recv_sem.at[which],
            device_id={"tp": device(dx, 0)},
            device_id_type=pl.DeviceIdType.MESH,
        )

    FIRST, REST, ALL = 0, 1, 2
    att_span = {FIRST: (0, late_at), REST: (late_at, att_rows), ALL: (0, att_rows)}
    mate_span = {FIRST: (0, mate_late), REST: (mate_late, mate_rows), ALL: (0, mate_rows)}
    cross_span = {FIRST: (0, early_rows), REST: (early_rows, rows), ALL: (0, rows)}

    def mate_slot(kind, c):
        return c if kind == FIRST else split + c

    def cross_slot(kind, c):
        return 0 if kind == FIRST else 1 + c

    def mate_item(kind, c):
        low, high = mate_span[kind]
        return mate_copy(low, high - low, c, mate_slot(kind, c))

    def multiply(kind, c):
        low, high = att_span[kind]
        product = jnp.dot(att[low:high], w_buf[c], preferred_element_type=jnp.float32)

        def part(first, count):
            return product[first - low : first - low + count]

        for dx in range(1, chips):
            if kind != REST and early:
                at = att_row(dx, 0, 0)
                keep[c, dx - 1, 0:early_rows] = part(at, early_rows)
                to = (dx - 1) * early_rows
                mate_send[c, to : to + early_rows] = part(at + early_rows, early_rows).astype(
                    jnp.bfloat16
                )
            if kind != FIRST:
                at = att_row(dx, 0, early)
                keep[c, dx - 1, early_rows:rows] = part(at, late_rows)
                to = mate_late + (dx - 1) * late_rows
                mate_send[c, to : to + late_rows] = part(at + late_rows, late_rows).astype(
                    jnp.bfloat16
                )
        if kind != REST:
            at = pl.multiple_of(c * columns, LANES)
            acc[:, :, pl.ds(at, columns)] = part(local_at, rows).reshape(seqs, draft, columns)
            mate_send[c, mate_local:mate_late] = part(local_at + rows, rows).astype(jnp.bfloat16)
        mate_item(kind, c).start()

    def pass_on(kind, c):
        mate_item(kind, c).wait_recv()
        low, high = cross_span[kind]
        for dx in range(1, chips):
            if kind != REST and early:
                at = (dx - 1) * early_rows
                both = keep[c, dx - 1, 0:early_rows] + mate_recv[c, at : at + early_rows].astype(
                    jnp.float32
                )
                cross_send[dx - 1, c, 0:early_rows] = both.astype(jnp.bfloat16)
            if kind != FIRST:
                at = mate_late + (dx - 1) * late_rows
                both = keep[c, dx - 1, early_rows:rows] + mate_recv[
                    c, at : at + late_rows
                ].astype(jnp.float32)
                cross_send[dx - 1, c, early_rows:rows] = both.astype(jnp.bfloat16)
            cross_copy(dx, low, high - low, c, cross_slot(kind, c)).start()
        if kind != REST:
            at = pl.multiple_of(c * columns, LANES)
            other = mate_recv[c, mate_local:mate_late].astype(jnp.float32)
            residual = res_buf[:, :, pl.ds(at, columns)].astype(jnp.float32)
            acc[:, :, pl.ds(at, columns)] += other.reshape(seqs, draft, columns) + residual

    res_copy.start()
    gain_copy.start()
    att_arrived(local_at + rows, rows, 2)
    if early:
        att_arrived(0, local_at, 0)
    res_copy.wait()

    def sweep(kind, first, last, pending, wait_late):
        lag = min(LAG, last - first)

        def step(c, carry):
            for k, (kind_before, c_before) in enumerate(pending):

                @pl.when(c - first == k)
                def _():
                    pass_on(kind_before, c_before)

            @pl.when(c - first >= lag)
            def _():
                pass_on(kind, c - lag)

            if wait_late:

                @pl.when(c == first)
                def _():
                    att_arrived(late_at, att_rows - late_at, 1)

            if kind != REST:
                w_copy(c).wait()
                if split:
                    later = split + c - jnp.minimum(c, 1)

                    @pl.when((c != 1) & (later < chunks))
                    def _():
                        w_copy(later).start()

            multiply(kind, c)
            return carry

        lax.fori_loop(first, last, step, 0)
        return [(kind, c) for c in range(last - lag, last)]

    sweeps = [(FIRST, 0, split), (ALL, split, chunks), (REST, 0, split)]
    sweeps = [x for x in sweeps if x[1] < x[2]]
    pending = []
    for index, (kind, low, high) in enumerate(sweeps):
        late_now = kind != FIRST and all(x[0] == FIRST for x in sweeps[:index])
        pending = sweep(kind, low, high, pending, late_now)
    for kind, c in pending:
        pass_on(kind, c)

    def arrived(kind, c, count):
        low, high = cross_span[kind]
        block = cross_recv.at[:, pl.ds(c, count), pl.ds(low, high - low)]
        pltpu.make_async_copy(block, block, cross_recv_sem.at[cross_slot(kind, c)]).wait()

    def collect(kind, c, squares):
        low, high = cross_span[kind]
        at = pl.multiple_of(c * columns, LANES)
        s0, s1 = low // draft, high // draft
        total = acc[s0:s1, :, pl.ds(at, columns)]
        for dx in range(1, chips):
            part = cross_recv[dx - 1, c, low:high].astype(jnp.float32)
            total = total + part.reshape(s1 - s0, draft, columns)
        acc[s0:s1, :, pl.ds(at, columns)] = total
        for tile in range(columns // LANES):
            part = total[:, :, tile * LANES : (tile + 1) * LANES]
            squares = squares + part * part
        return squares

    gain_copy.wait()
    wide_gain[...] = gain_buf[...].astype(jnp.float32)

    def finish(kind, c, squares):
        arrived(kind, c, 1)
        return collect(kind, c, squares)

    sums = {
        FIRST: jnp.zeros((early, draft, LANES), jnp.float32) if early else None,
        REST: jnp.zeros((late, draft, LANES), jnp.float32),
        ALL: jnp.zeros((seqs, draft, LANES), jnp.float32),
    }
    for kind, low, high in sweeps:
        if kind == FIRST:
            arrived(FIRST, 0, split)
        do = collect if kind == FIRST else finish
        sums[kind] = lax.fori_loop(low, high, functools.partial(do, kind), sums[kind])
    squares = sums[ALL]
    if split:
        squares = squares + jnp.concatenate([sums[FIRST], sums[REST]], axis=0)
    mean = jnp.sum(squares, axis=-1, keepdims=True) / model
    scale_ref[...] = jnp.broadcast_to(lax.rsqrt(mean + 1e-05), scale_ref.shape)

    pltpu.make_async_copy(att_send, att_send, att_send_sem).wait()
    pltpu.make_async_copy(mate_send, mate_send, mate_send_sem).wait()
    pltpu.make_async_copy(cross_send, cross_send, cross_send_sem).wait()


def on_device(n, queries, kv_cache, lengths, residual, out_weight, norm_gain):
    seqs, draft, width = queries.shape
    kv_heads, slots_kv, pair_dim = kv_cache.shape[1:]
    head_dim = pair_dim // 2
    heads = width // head_dim
    depth, model = out_weight.shape
    chips = n // CORES
    others = max(1, chips - 1)
    rows = seqs * draft
    columns = math.gcd(model, COLUMNS)
    chunks = model // columns
    split = chunks * 3 // 8 if seqs > 1 and chips > 1 and chunks % 2 == 0 else 0
    kv_per_dest = max(1, kv_heads // n)
    bf16, f32 = jnp.bfloat16, jnp.float32
    dma = pltpu.SemaphoreType.DMA
    summed, scale, gain = pl.pallas_call(
        functools.partial(block_kernel, n, split),
        out_shape=(
            pltpu.VMEM(residual.shape, f32),
            pltpu.VMEM((seqs, draft, LANES), f32),
            pltpu.VMEM(norm_gain.shape, f32),
        ),
        in_specs=[pl.BlockSpec(memory_space=pl.ANY)] * 6,
        out_specs=[pl.BlockSpec(memory_space=pltpu.VMEM)] * 3,
        scratch_shapes=[
            pltpu.SMEM(lengths.shape, jnp.int32),
            pltpu.VMEM(norm_gain.shape, bf16),
            pltpu.VMEM(queries.shape, bf16),
            pltpu.VMEM((n * seqs, kv_per_dest, slots_kv, pair_dim), bf16),
            pltpu.VMEM(residual.shape, bf16),
            pltpu.VMEM((chunks, depth, columns), bf16),
            pltpu.VMEM((n - 1, rows, depth), bf16),
            pltpu.VMEM((n * rows, depth), bf16),
            pltpu.VMEM((chunks, others, rows, columns), f32),
            pltpu.VMEM((chunks, chips * rows, columns), bf16),
            pltpu.VMEM((chunks, chips * rows, columns), bf16),
            pltpu.VMEM((others, chunks, rows, columns), bf16),
            pltpu.VMEM((others, chunks, rows, columns), bf16),
            dma((3,)),
            dma((seqs,)),
            dma((n * seqs,)),
            dma((chunks,)),
            dma,
            dma((3,)),
            dma,
            dma((chunks + split,)),
            dma,
            dma((1 + chunks,)),
        ],
        compiler_params=pltpu.CompilerParams(
            collective_id=0, has_side_effects=True, vmem_limit_bytes=56 * 1024 * 1024
        ),
    )(lengths, queries, kv_cache, residual, out_weight, norm_gain)
    normed = summed * scale[:, :, :1] * gain
    return summed.astype(bf16), normed.astype(bf16)


def solution(mesh):
    return jax.shard_map(
        functools.partial(on_device, mesh.shape["tp"]),
        mesh=mesh,
        in_specs=(
            P(("dp", "tp"), None, None),
            P(("dp", "tp"), None, None, None),
            P(("dp", "tp")),
            P(("dp", "tp"), None, None),
            P("tp", None),
            P(),
        ),
        out_specs=(P(("dp", "tp"), None, None), P(("dp", "tp"), None, None)),
        check_vma=False,
    )
```
